8 devices in a mesh: dp: 1 (over z), tp: 8 (over x, y, core).
Axes of the slice: x: 2, y: 2, z: 1, core: 2. Of those that a mesh axis runs over, the one named last changes fastest.
Arguments:
- x: bfloat16 [4096, 2048], P(('dp', 'tp'))
- dy: bfloat16 [4096, 2048], P(('dp', 'tp'))
- gate: bfloat16 [4096, 6144], P('dp', 'tp')
- up: bfloat16 [4096, 6144], P('dp', 'tp')
- w_gate: bfloat16 [2048, 6144], P(None, 'tp')
- w_up: bfloat16 [2048, 6144], P(None, 'tp')
- w_down: bfloat16 [6144, 2048], P('tp')
Outputs:
- output 1: bfloat16 [4096, 2048], P(('dp', 'tp'))
- output 2: bfloat16 [2048, 6144], P('dp', 'tp')
- output 3: bfloat16 [2048, 6144], P('dp', 'tp')
- output 4: bfloat16 [6144, 2048], P(('dp', 'tp'))
All inputs are finite; a program needn't handle non-finite values.
Results may differ from the reference program's by a relative error of at most 0.012.
Values are sent between devices in bfloat16 or wider.
A program may use at most 2 GiB of HBM per device.

```python
import jax
import jax.numpy as jnp

ROWS = 4096
D = 2048
FF = 6144


def act(gate, up):
    return jax.nn.silu(gate) * up


def setup_inputs(seed: int = 0, part: int = 0) -> dict:
    kx, ky, ka, kb, kg, ku, kd = jax.random.split(jax.random.key(seed), 7)
    kx, ky, ka, kb = (jax.random.fold_in(k, part) for k in (kx, ky, ka, kb))
    drawn = {
        "x": jax.random.normal(kx, (ROWS, D), jnp.float32),
        "dy": jax.random.normal(ky, (ROWS, D), jnp.float32),
        "gate": jax.random.normal(ka, (ROWS, FF), jnp.float32),
        "up": jax.random.normal(kb, (ROWS, FF), jnp.float32),
        "w_gate": jax.random.normal(kg, (D, FF), jnp.float32) * D**-0.5,
        "w_up": jax.random.normal(ku, (D, FF), jnp.float32) * D**-0.5,
        "w_down": jax.random.normal(kd, (FF, D), jnp.float32) * FF**-0.5,
    }
    return {k: v.astype(jnp.bfloat16) for k, v in drawn.items()}


def reference(x, dy, gate, up, w_gate, w_up, w_down):
    hidden, back = jax.vjp(act, gate.astype(jnp.float32), up.astype(jnp.float32))
    d_hidden = jnp.dot(dy, w_down.T, preferred_element_type=jnp.float32)
    d_gate, d_up = (g.astype(jnp.bfloat16) for g in back(d_hidden))
    dx = jnp.dot(d_gate, w_gate.T, preferred_element_type=jnp.float32) + jnp.dot(d_up, w_up.T, preferred_element_type=jnp.float32)
    dw_gate = jnp.dot(x.T, d_gate, preferred_element_type=jnp.float32)
    dw_up = jnp.dot(x.T, d_up, preferred_element_type=jnp.float32)
    dw_down = jnp.dot(hidden.astype(jnp.bfloat16).T, dy, preferred_element_type=jnp.float32)
    return tuple(g.astype(jnp.bfloat16) for g in (dx, dw_gate, dw_up, dw_down))
```

```python
import functools

import jax
import jax.numpy as jnp
from jax import lax
from jax.experimental import pallas as pl
from jax.experimental.pallas import tpu as pltpu
from jax.sharding import PartitionSpec as P

F32, BF16 = jnp.float32, jnp.bfloat16
X, Y, S = 4, 2, 1
NT = (((1,), (1,)), ((), ()))
TN = (((0,), (0,)), ((), ()))


def send(a, k, name):
    with jax.named_scope(name):
        return lax.ppermute(a, "tp", [(i, i ^ k) for i in range(8)])


def token_kernel(parts, n_r, kinds, owner, *refs):
    dys, (gate, up, wd, wg, wu), refs = refs[:parts], refs[parts : parts + 5], refs[parts + 5 :]
    rs, (dg_out, du_out, h_out), dxs = refs[:n_r], refs[n_r : n_r + 3], refs[n_r + 3 :]
    step = pl.program_id(0)
    dy = dys[0][...] if parts == 1 else jnp.where(step == 0, dys[0][...], dys[1][...])
    dh = lax.dot_general(dy, wd[...], NT, preferred_element_type=F32)
    g, u = gate[...].astype(F32), up[...].astype(F32)
    sig = jax.nn.sigmoid(g)
    silu = g * sig
    h_out[...] = (silu * u).astype(BF16)
    du = (dh * silu).astype(BF16)
    dg = (dh * u * (sig + silu * (1.0 - sig))).astype(BF16)
    du_out[...] = du
    dg_out[...] = dg
    dx = lax.dot_general(dg, wg[...], NT, preferred_element_type=F32)
    dx += lax.dot_general(du, wu[...], NT, preferred_element_type=F32)
    if n_r:
        dx += rs[0][...].astype(F32)
    if len(kinds) == 1:
        dxs[0][...] = dx.astype(kinds[0])
    else:
        for half in range(2):
            @pl.when(step == half)
            def _(half=half):
                dxs[half][...] = dx.astype(kinds[half])


def token_block(owner, dys, gate, up, wd, wg, wu, r, kinds, name):
    tile = 256
    d, f = wg.shape
    rows = 512
    whole = lambda a: pl.BlockSpec(a.shape, lambda i, o: (0,) * a.ndim, pipeline_mode=pl.Buffered(1))
    by_tile = lambda w: pl.BlockSpec((tile, w), lambda i, o: (i, 0))
    mine = pl.BlockSpec((tile, f), lambda i, o: (o[0] * (rows // tile) + i, 0))
    dy_specs = [by_tile(d)] if len(dys) == 1 else [whole(dys[0])] * 2
    r_in = [] if r is None else [r]
    if len(kinds) == 1:
        dx_specs, dx_shapes = [by_tile(d)], [jax.ShapeDtypeStruct((rows, d), kinds[0])]
    else:
        dx_specs = [pl.BlockSpec((tile, d), lambda i, o: (0, 0))] * 2
        dx_shapes = [jax.ShapeDtypeStruct((tile, d), k) for k in kinds]
    with jax.named_scope(name):
        return pl.pallas_call(
            functools.partial(token_kernel, len(dys), len(r_in), kinds),
            grid_spec=pltpu.PrefetchScalarGridSpec(
                num_scalar_prefetch=1,
                grid=(rows // tile,),
                in_specs=dy_specs + [mine, mine, whole(wd), whole(wg), whole(wu)] + [by_tile(d)] * len(r_in),
                out_specs=[by_tile(f)] * 3 + dx_specs,
            ),
            out_shape=[jax.ShapeDtypeStruct((rows, f), BF16)] * 3 + dx_shapes,
            cost_estimate=pl.CostEstimate(flops=6 * rows * d * f, bytes_accessed=16 << 20, transcendentals=rows * f),
            name=name,
        )(owner, *dys, gate, up, wd, wg, wu, *r_in)


def weight_kernel(n_a, n_b, *refs):
    a_refs, b_refs, out = refs[:n_a], refs[n_a : n_a + n_b], refs[-1]
    pieces = []
    for ref in a_refs:
        pieces += [ref[...]]
    right, at, where = [], 0, 0
    for ref in b_refs:
        right.append(ref[...])
    total = None
    i = j = 0
    a_off = b_off = 0
    while i < n_a:
        n = min(pieces[i].shape[0] - a_off, right[j].shape[0] - b_off)
        t = lax.dot_general(pieces[i][a_off : a_off + n], right[j][b_off : b_off + n], TN, preferred_element_type=F32)
        total = t if total is None else total + t
        a_off, b_off = a_off + n, b_off + n
        if a_off == pieces[i].shape[0]:
            i, a_off = i + 1, 0
        if b_off == right[j].shape[0]:
            j, b_off = j + 1, 0
    out[...] = total.astype(out.dtype)


def weight_grad(a_list, b_list, tile, name):
    m, n = a_list[0].shape[1], b_list[0].shape[1]
    rows = sum(a.shape[0] for a in a_list)
    with jax.named_scope(name):
        return pl.pallas_call(
            functools.partial(weight_kernel, len(a_list), len(b_list)),
            grid=(m // tile,),
            in_specs=[pl.BlockSpec((a.shape[0], tile), lambda i: (0, i)) for a in a_list]
            + [pl.BlockSpec(b.shape, lambda i: (0, 0), pipeline_mode=pl.Buffered(1)) for b in b_list],
            out_specs=pl.BlockSpec((tile, n), lambda i: (i, 0)),
            out_shape=jax.ShapeDtypeStruct((m, n), BF16),
            cost_estimate=pl.CostEstimate(flops=2 * rows * m * n, bytes_accessed=30 << 20, transcendentals=0),
            name=name,
        )(*a_list, *b_list)


def final_kernel(own_a, own_b, xa, xb, ya, yb, out):
    for half, (own, x, y) in enumerate(((own_a, xa, ya), (own_b, xb, yb))):
        out[half] = (own[...] + x[...].astype(F32) + y[...].astype(F32)).astype(BF16)


def final_sum(own_a, own_b, xa, xb, ya, yb):
    n, d = own_a.shape
    tile = 64
    spec = pl.BlockSpec((tile, d), lambda i: (i, 0))
    with jax.named_scope("final"):
        out = pl.pallas_call(
            final_kernel,
            grid=(n // tile,),
            in_specs=[spec] * 6,
            out_specs=pl.BlockSpec((2, tile, d), lambda i: (0, i, 0)),
            out_shape=jax.ShapeDtypeStruct((2, n, d), BF16),
            cost_estimate=pl.CostEstimate(flops=6 * n * d, bytes_accessed=16 * n * d, transcendentals=0),
            name="final",
        )(own_a, own_b, xa, xb, ya, yb)
    return out.reshape(2 * n, d)


def body(x, dy, gate, up, wg, wu, wd):
    me = lax.axis_index("tp")
    own = lambda b: jnp.reshape(jnp.bitwise_xor(me, b), (1,)).astype(jnp.int32)
    block = lambda b, dys, r, kinds: token_block(own(b), dys, gate, up, wd, wg, wu, r, kinds, f"tok{b}")
    h = 256
    top, bot = x[:h], x[h:]

    d4, d2, d1 = send(dy, X, "dy_x"), send(dy, Y, "dy_y"), send(dy, S, "dy_s")
    x4a, x2b = send(top, X, "xa_x"), send(bot, Y, "xb_y")
    x1 = send(x, S, "x_s")

    g1, u1, h1, t1 = block(1, [d1], None, (BF16,))
    r0 = send(t1, S, "r0")
    g0, u0, h0, c0a, c0b = block(0, [dy], r0, (F32, F32))

    d6a, d6b = send(d4[:h], Y, "dyf_y"), send(d2[h:], X, "dyf_x")
    d5, d3 = send(d4, S, "d5"), send(d2, S, "d3")
    x4b, x2a = send(bot, X, "xb_x"), send(top, Y, "xa_y")

    g5, u5, h5, t5 = block(5, [d5], None, (BF16,))
    r4 = send(t5, S, "r4")
    g3, u3, h3, t3 = block(3, [d3], None, (BF16,))
    r2 = send(t3, S, "r2")
    g4, u4, h4, c4a, c4b = block(4, [d4], r4, (BF16, F32))
    g2, u2, h2, c2a, c2b = block(2, [d2], r2, (F32, BF16))

    x6a, x6b = send(x4a, Y, "xf_y"), send(x2b, X, "xf_x")
    x5a, x3b = send(x4a, S, "x5a"), send(x2b, S, "x3b")
    d7a, d7b = send(d6a, S, "d7a"), send(d6b, S, "d7b")
    g7, u7, h7, t7 = block(7, [d7a, d7b], None, (BF16,))
    r6 = send(t7, S, "r6")
    g6, u6, h6, c6a, c6b = block(6, [d6a, d6b], r6, (BF16, BF16))
    e2a, e4b = send(c6a, X, "rs1_x"), send(c6b, Y, "rs1_y")

    x5b, x3a = send(x4b, S, "x5b"), send(x2a, S, "x3a")
    dwd = weight_grad([h0, h1, h2, h3, h4, h5, h6, h7], [dy, d1, d2, d3, d4, d5, d6a, d6b, d7a, d7b], 256, "dw_down")

    fxa, fyb = send(c4a, X, "rs2_xa"), send(c2b, Y, "rs2_yb")
    x7a, x7b = send(x6a, S, "x7a"), send(x6b, S, "x7b")
    xs = [x, x1, x2a, x2b, x3a, x3b, x4a, x4b, x5a, x5b, x6a, x6b, x7a, x7b]
    dwg = weight_grad(xs, [g0, g1, g2, g3, g4, g5, g6, g7], 512, "dw_gate")
    with jax.named_scope("rs_add"):
        s4b = (c4b + e4b.astype(F32)).astype(BF16)
        s2a = (c2a + e2a.astype(F32)).astype(BF16)
    fxb, fya = send(s4b, X, "rs2_xb"), send(s2a, Y, "rs2_ya")
    dwu = weight_grad(xs, [u0, u1, u2, u3, u4, u5, u6, u7], 512, "dw_up")

    dx = final_sum(c0a, c0b, fxa, fxb, fya, fyb)
    return dx, dwg, dwu, dwd


def solution(mesh):
    rows, cols = P(("dp", "tp"), None), P(None, "tp")
    both = P("dp", "tp")
    return jax.shard_map(
        body,
        mesh=mesh,
        in_specs=(rows, rows, both, both, cols, cols, P("tp", None)),
        out_specs=(rows, both, both, rows),
        check_vma=False,
    )
```

```python
import functools

import jax
import jax.numpy as jnp
from jax import lax
from jax.experimental import pallas as pl
from jax.experimental.pallas import tpu as pltpu
from jax.sharding import PartitionSpec as P


TILE = 256
CUT = 256
F32, BF16 = jnp.float32, jnp.bfloat16
X, Y, S = 4, 2, 1
NT = (((1,), (1,)), ((), ()))
TN = (((0,), (0,)), ((), ()))


def partner(i, b):
    return i ^ (b ^ 6 if i & 1 and b & 6 in (2, 4) else b)


def send(a, b):
    return lax.ppermute(a, "tp", [(i, partner(i, b)) for i in range(8)])


def token_kernel(n_dy, owners, *refs):
    dys, (gate, up, wd_hbm, wg_hbm, wu_hbm), refs = refs[:n_dy], refs[n_dy : n_dy + 5], refs[n_dy + 5 :]
    gu_out, h_out, theirs, ours, dy_buf, wd, wgu, dy_sem, w_sem = refs
    step, steps = pl.program_id(0), pl.num_programs(0)
    f = wd.shape[0]
    pieces = [(ref, at) for ref in dys for at in range(0, ref.shape[0], TILE)]

    def fetch(n):
        for p, (ref, at) in enumerate(pieces):
            @pl.when(n == p)
            def _(p=p, ref=ref, at=at):
                pltpu.make_async_copy(ref.at[pl.ds(at, TILE)], dy_buf.at[p % 2], dy_sem.at[p % 2]).start()

    targets = (wd_hbm, wd), (wg_hbm, wgu.at[:, pl.ds(0, f)]), (wu_hbm, wgu.at[:, pl.ds(f, f)])
    weights = [pltpu.make_async_copy(src, dst, w_sem.at[n]) for n, (src, dst) in enumerate(targets)]

    @pl.when(step == 0)
    def _():
        fetch(0)
        for w in weights:
            w.start()

    fetch(step + 1)
    slot = lax.rem(step, 2)
    pltpu.make_async_copy(dys[0].at[pl.ds(0, TILE)], dy_buf.at[slot], dy_sem.at[slot]).wait()

    def tile(first, dx_out):
        if first:
            pl.when(step == 0)(weights[0].wait)
        dh = lax.dot_general(dy_buf[slot], wd[...], NT, preferred_element_type=F32)
        g, u = gate[...].astype(F32), up[...].astype(F32)
        sig = jax.nn.sigmoid(g)
        silu = g * sig
        h_out[...] = (silu * u).astype(BF16)
        gu_out[:, :f] = (dh * u * (sig + silu * (1.0 - sig))).astype(BF16)
        gu_out[:, f:] = (dh * silu).astype(BF16)
        if first:
            pl.when(step == 0)(weights[1].wait)
            pl.when(step == 0)(weights[2].wait)
        dx_out[...] = lax.dot_general(gu_out[...], wgu[...], NT, preferred_element_type=F32).astype(dx_out.dtype)

    pl.when(step < steps // 2)(lambda: tile(True, theirs))
    pl.when(step >= steps // 2)(lambda: tile(False, ours))


def token_blocks(owners, dys, gate, up, wd, wg, wu):
    d, f = wg.shape
    rows = sum(a.shape[0] for a in dys)
    steps, per = rows // TILE, rows // TILE // owners.shape[0]
    half = steps // 2
    hbm = pl.BlockSpec(memory_space=pl.ANY)
    mine = pl.BlockSpec((TILE, f), lambda i, o: (o[i // per] * per + i % per, 0))
    by_tile = pl.BlockSpec((TILE, f), lambda i, o: (i, 0))
    return pl.pallas_call(
        functools.partial(token_kernel, len(dys)),
        grid_spec=pltpu.PrefetchScalarGridSpec(
            num_scalar_prefetch=1,
            grid=(steps,),
            in_specs=[hbm] * len(dys) + [mine, mine] + [hbm] * 3,
            out_specs=[pl.BlockSpec((TILE, 2 * f), lambda i, o: (i, 0)), by_tile]
            + [
                pl.BlockSpec((TILE, d), lambda i, o: (jnp.minimum(i, half - 1), 0)),
                pl.BlockSpec((TILE, d), lambda i, o: (jnp.maximum(i - half, 0), 0)),
            ],
            scratch_shapes=[pltpu.VMEM((2, TILE, d), BF16)]
            + [pltpu.VMEM((f, d), BF16), pltpu.VMEM((d, 2 * f), BF16)]
            + [pltpu.SemaphoreType.DMA((2,)), pltpu.SemaphoreType.DMA((3,))],
        ),
        out_shape=[jax.ShapeDtypeStruct((rows, 2 * f), BF16), jax.ShapeDtypeStruct((rows, f), BF16)]
        + [jax.ShapeDtypeStruct((rows // 2, d), BF16), jax.ShapeDtypeStruct((rows // 2, d), F32)],
        cost_estimate=pl.CostEstimate(flops=6 * rows * d * f, bytes_accessed=10 * rows * d, transcendentals=rows * f),
    )(owners, *dys, gate, up, wd, wg, wu)


PART = 512
COLS = 256


def weight_kernel(n_held, n_streamed, n_sofar, outs, *refs):
    held, refs = refs[:n_held], refs[n_held:]
    streamed, refs = refs[:n_streamed], refs[n_streamed:]
    sofar, refs = refs[:n_sofar], refs[n_sofar:]
    out, (held_buf, buf, acc, held_sem, sem) = refs[:outs], refs[outs:]
    step, steps = pl.program_id(0), pl.num_programs(0)
    rows, f = held_buf.shape
    parts = rows // PART

    def start_held(n):
        row = 0
        for ref in held:
            size = min(ref.shape[0], PART)
            for at in range(0, ref.shape[0], size):
                if row // PART == n:
                    dst = held_buf.at[pl.ds(row, size)]
                    pltpu.make_async_copy(ref.at[pl.ds(at, size)], dst, held_sem.at[n]).start()
                row += size

    def start_streamed(i, slot, n=None):
        row = 0
        cols = pl.ds(pl.multiple_of(i * COLS, COLS), COLS)
        for ref in streamed:
            size = min(ref.shape[0], PART)
            for at in range(0, ref.shape[0], size):
                if n is None or row // PART == n:
                    dst = buf.at[slot, pl.ds(row, size)]
                    pltpu.make_async_copy(ref.at[pl.ds(at, size), cols], dst, sem.at[slot, row // PART]).start()
                row += size

    def wait(slot, n):
        here = buf.at[slot, pl.ds(n * PART, PART)]
        pltpu.make_async_copy(here, here, sem.at[slot, n]).wait()

    def dot(held_part, streamed_part):
        return lax.dot_general(streamed_part, held_part, TN, preferred_element_type=F32)

    def store(total):
        for n, ref in enumerate(out):
            cols = slice(n * (f // outs), (n + 1) * (f // outs))
            part = total[:, cols]
            if sofar:
                part += sofar[0][:, cols]
            ref[...] = part.astype(ref.dtype)

    slot = lax.rem(step, 2)

    @pl.when(step == 0)
    def _():
        for n in range(parts):
            start_streamed(0, 0, n)
            start_held(n)
        start_streamed(1, 1)
        for n in range(parts):
            at = pl.ds(n * PART, PART)
            wait(0, n)
            there = held_buf.at[at]
            pltpu.make_async_copy(there, there, held_sem.at[n]).wait()
            term = dot(held_buf[at], buf[0, at])
            if n:
                term += acc[...]
            if n < parts - 1:
                acc[...] = term
            else:
                store(term)

    @pl.when(step > 0)
    def _():
        @pl.when(step + 1 < steps)
        def _():
            start_streamed(step + 1, 1 - slot)

        for n in range(parts):
            wait(slot, n)
        store(dot(held_buf[...], buf[slot]))


def weight_grad(held, streamed, outs, sofar=(), dtype=BF16, vmem=60 << 20):
    rows = sum(a.shape[0] for a in held)
    f, d = held[0].shape[1], streamed[0].shape[1]
    hbm = pl.BlockSpec(memory_space=pl.ANY)
    return pl.pallas_call(
        functools.partial(weight_kernel, len(held), len(streamed), len(sofar), outs),
        grid=(d // COLS,),
        in_specs=[hbm] * (len(held) + len(streamed))
        + [pl.BlockSpec((COLS, f), lambda i: (i, 0))] * len(sofar),
        out_specs=[pl.BlockSpec((COLS, f // outs), lambda i: (i, 0))] * outs,
        out_shape=[jax.ShapeDtypeStruct((d, f // outs), dtype)] * outs,
        scratch_shapes=[
            pltpu.VMEM((rows, f), BF16),
            pltpu.VMEM((2, rows, COLS), BF16),
            pltpu.VMEM((COLS, f), F32),
            pltpu.SemaphoreType.DMA((rows // PART,)),
            pltpu.SemaphoreType.DMA((2, rows // PART)),
        ],
        compiler_params=pltpu.CompilerParams(vmem_limit_bytes=vmem),
        cost_estimate=pl.CostEstimate(flops=2 * rows * f * d, bytes_accessed=30 << 20, transcendentals=0),
    )(*held, *streamed, *sofar)


def add_kernel(sizes, *refs):
    outs, at = refs[sum(sizes) :], 0
    for out, size in zip(outs, sizes):
        total = refs[at][...].astype(F32)
        for ref in refs[at + 1 : at + size]:
            total += ref[...].astype(F32)
        out[...] = total.astype(out.dtype)
        at += size


def add(sums, rows, dtype):
    tile = 128 if rows % 128 == 0 else END
    d = sums[0][0][0].shape[1]
    terms = [term for one in sums for term in one]
    specs = [pl.BlockSpec((tile, d), lambda i, first=first // tile: (first + i, 0)) for _, first in terms]
    return pl.pallas_call(
        functools.partial(add_kernel, [len(one) for one in sums]),
        grid=(rows // tile,),
        in_specs=specs,
        out_specs=[pl.BlockSpec((tile, d), lambda i: (i, 0))] * len(sums),
        out_shape=[jax.ShapeDtypeStruct((rows, d), dtype)] * len(sums),
        cost_estimate=pl.CostEstimate(flops=4 * rows * d, bytes_accessed=16 * rows * d, transcendentals=0),
    )(*[a for a, _ in terms])


END = 64


def final_kernel(own_a, own_b, xa, xb, ya, yb, *refs):
    out = refs[-1]
    out[0] = (own_a[...] + xa[...].astype(F32) + ya[...].astype(F32)).astype(BF16)
    out[1] = (own_b[...] + xb[...].astype(F32) + yb[...].astype(F32)).astype(BF16)


def final_sum(terms, first, rows, sofar):
    half, d = terms[0][0].shape
    spec = lambda at: pl.BlockSpec((END, d), lambda i: (at // END + i, 0))
    return pl.pallas_call(
        final_kernel,
        grid=(rows // END,),
        in_specs=[spec(at) for _, at in terms] + [pl.BlockSpec(memory_space=pl.ANY)] * len(sofar),
        out_specs=pl.BlockSpec((2, END, d), lambda i: (0, first // END + i, 0)),
        out_shape=jax.ShapeDtypeStruct((2, half, d), BF16),
        input_output_aliases={len(terms): 0} if sofar else {},
        compiler_params=pltpu.CompilerParams(vmem_limit_bytes=36 << 20),
        cost_estimate=pl.CostEstimate(flops=6 * rows * d, bytes_accessed=20 * rows * d, transcendentals=0),
    )(*[a for a, _ in terms], *sofar)


def layer(x, dy, gate, up, wg, wu, wd):
    me = lax.axis_index("tp")

    def tokens(blocks, dys):
        even, odd = ([partner(core, b) ^ core for b in blocks] for core in range(2))
        owners = me ^ jnp.where(me % 2 == 0, jnp.array(even, jnp.int32), jnp.array(odd, jnp.int32))
        return token_blocks(owners, dys, gate, up, wd, wg, wu)

    h = 256
    top, bot = x[:CUT], x[CUT:]

    d4, d2, d1 = send(dy, X), send(dy, Y), send(dy, S)
    x4a, x2b = send(top, X), send(bot, Y)
    x1 = send(x, S)
    gu10, h10, t1, c0 = tokens([1, 0], [d1, dy])
    r0 = send(t1, S)

    first_gu = weight_grad([gu10], [x1, x], 1, dtype=F32)

    own_a, own_b = add([[(c0, 0), (r0, 0)], [(c0, h), (r0, h)]], h, F32)
    d4_top, d2_bot = add([[(d4, 0)], [(d2, h)]], h, BF16)
    d6a, d6b = send(d4_top, Y), send(d2_bot, X)
    d3, d5 = send(d4, S), send(d2, S)
    x4b, x2a = send(bot, X), send(top, Y)
    gu42, h42, t35, c42 = tokens([3, 5, 4, 2], [d3, d5, d4, d2])
    r42 = send(t35, S)

    x6a, x6b = send(x4a, Y), send(x2b, X)
    x3a, x5b = send(x4a, S), send(x2b, S)
    d7a, d7b = send(d6a, S), send(d6b, S)
    gu76, h76, t7, c6 = tokens([7, 6], [d7a, d7b, d6a, d6b])
    r6 = send(t7, S)
    p6a, p6b = add([[(c6, 0), (r6, 0)], [(c6, h), (r6, h)]], h, BF16)
    e2a, e4b = send(p6a, X), send(p6b, Y)
    p4a, p2b = add([[(c42, 0), (r42, 0)], [(c42, 3 * h), (r42, 3 * h)]], h, BF16)
    fxa, fyb = send(p4a, X), send(p2b, Y)

    x3b, x5a = send(x4b, S), send(x2a, S)
    (dwd,) = weight_grad([d1, dy, d3, d5, d4, d2, d7a, d7b, d6a, d6b], [h10, h42, h76], 1, vmem=56 << 20)
    main = h - END
    s4b, s2a = add([[(c42, h), (r42, h), (e4b, 0)], [(c42, 2 * h), (r42, 2 * h), (e2a, 0)]], main, BF16)
    fxb, fya = send(s4b, X), send(s2a, Y)
    near_end = [[(c42, h + main), (r42, h + main), (e4b, main)], [(c42, 2 * h + main), (r42, 2 * h + main), (e2a, main)]]
    t4b, t2a = add(near_end, END, BF16)
    gxb, gya = send(t4b, X), send(t2a, Y)

    x7a, x7b = send(x6a, S), send(x6b, S)
    xs = [x3a, x3b, x5a, x5b, x4a, x4b, x2a, x2b, x7a, x7b, x6a, x6b]
    dwg, dwu = weight_grad([gu42, gu76], xs, 2, first_gu)
    dx = final_sum([(t, 0) for t in (own_a, own_b, fxa, fxb, fya, fyb)], 0, main, ())
    last = [(own_a, main), (own_b, main), (fxa, main), (gxb, 0), (gya, 0), (fyb, main)]
    dx = final_sum(last, main, END, (dx,))
    return dx.reshape(2 * h, -1), dwg, dwu, dwd


def solution(mesh):
    rows, cols = P(("dp", "tp"), None), P(None, "tp")
    both = P("dp", "tp")
    return jax.shard_map(
        layer,
        mesh=mesh,
        in_specs=(rows, rows, both, both, cols, cols, P("tp", None)),
        out_specs=(rows, both, both, rows),
        check_vma=False,
    )
```
